64 devices in a mesh: rep: 8 (over x, y, core), dp: 8 (over z).
Axes of the slice: x: 2, y: 2, z: 8, core: 2. Of those that a mesh axis runs over, the one named last changes fastest.
The devices are a block of a 4x4x8 slice.
Arguments:
- x: bfloat16 [64, 4096, 512], P(('rep', 'dp')), parts along dimension 0
- dy: bfloat16 [64, 4096, 512], P(('rep', 'dp')), parts along dimension 0
- w_gate: bfloat16 [2, 512, 1408], P(None, 'dp')
- w_up: bfloat16 [2, 512, 1408], P(None, 'dp')
- w_down: bfloat16 [2, 1408, 512], P(None, 'dp')
- m_w_gate: float32 [2, 512, 1408], P(None, 'dp')
- m_w_up: float32 [2, 512, 1408], P(None, 'dp')
- m_w_down: float32 [2, 1408, 512], P(None, 'dp')
- v_w_gate: float32 [2, 512, 1408], P(None, 'dp')
- v_w_up: float32 [2, 512, 1408], P(None, 'dp')
- v_w_down: float32 [2, 1408, 512], P(None, 'dp')
Outputs:
- output 1: bfloat16 [16, 512, 1408], P('rep', 'dp'), parts along dimension 0
- output 2: bfloat16 [16, 512, 1408], P('rep', 'dp'), parts along dimension 0
- output 3: bfloat16 [16, 1408, 512], P('rep', 'dp'), parts along dimension 0
- output 4: float32 [16, 512, 1408], P('rep', 'dp'), parts along dimension 0
- output 5: float32 [16, 512, 1408], P('rep', 'dp'), parts along dimension 0
- output 6: float32 [16, 1408, 512], P('rep', 'dp'), parts along dimension 0
- output 7: float32 [16, 512, 1408], P('rep', 'dp'), parts along dimension 0
- output 8: float32 [16, 512, 1408], P('rep', 'dp'), parts along dimension 0
- output 9: float32 [16, 1408, 512], P('rep', 'dp'), parts along dimension 0
There are 8 independent parts. The reference program is written for one: setup_inputs(seed, part) draws one part's arguments, and reference() takes and returns one part's arrays. A program takes and returns all parts, laid end to end along the dimension named above; an argument that names none is the same for every part.
All inputs are finite; a program needn't handle non-finite values.
Results may differ from the reference program's by a relative error of at most 0.022.
Values are sent between devices in bfloat16 or wider.
A program may use at most 768 MiB of HBM per device.

```python
import jax
import jax.numpy as jnp
from jax import lax

SEQUENCES = 8
TOKENS = 4096
D = 512
FF = 1408
LAYERS = 2
NAMES = ("w_gate", "w_up", "w_down")
SHAPES = {"w_gate": (LAYERS, D, FF), "w_up": (LAYERS, D, FF), "w_down": (LAYERS, FF, D)}


def bump(key, n, height):
    away = (jnp.arange(n, dtype=jnp.int32) - jax.random.randint(key, (), 0, n, jnp.int32)) % n
    return jnp.where(away < n // 8, height, 1.0)


def together(key, own, strength):
    shared = jax.random.normal(key, own.shape[1:], jnp.float32)
    return (own + strength * shared) * lax.rsqrt(1 + strength * strength)


def setup_inputs(seed: int = 0, part: int = 0) -> dict:
    kx, kdy, ka, kb, kz, kf, kh, kl, *keys = jax.random.split(jax.random.key(seed), 8 + 3 * len(NAMES))
    kx, kdy, ka, kb = (jax.random.fold_in(k, part) for k in (kx, kdy, ka, kb))
    kw, km, kv = (keys[i::3] for i in range(3))
    shape = (SEQUENCES, TOKENS, D)
    much_x, much_dy = jax.random.uniform(kz, (2,), jnp.float32, 0.0, 1.0)
    loud = 2.0 ** jax.random.uniform(jax.random.fold_in(kz, 1), (), jnp.float32, -1.0, 2.0)
    layers = 2.0 ** jax.random.uniform(kl, (LAYERS, 1, 1), jnp.float32, -1.0, 1.0)
    x = together(ka, jax.random.normal(kx, shape, jnp.float32), much_x) * bump(kf, D, 4.0)
    dy = together(kb, jax.random.normal(kdy, shape, jnp.float32), much_dy)
    drawn = {"x": x.astype(jnp.bfloat16), "dy": (loud * dy * (SEQUENCES * TOKENS) ** -0.5).astype(jnp.bfloat16)}
    for key, name in zip(kw, NAMES, strict=True):
        w = jax.random.normal(key, SHAPES[name], jnp.float32) * SHAPES[name][1] ** -0.5
        drawn[name] = (w * {"w_gate": 1.0, "w_up": bump(kh, FF, 4.0), "w_down": layers}[name]).astype(jnp.bfloat16)
    for key, name in zip(km, NAMES, strict=True):
        drawn[f"m_{name}"] = 0.1 * jax.random.normal(key, SHAPES[name], jnp.float32)
    for key, name in zip(kv, NAMES, strict=True):
        drawn[f"v_{name}"] = jax.random.uniform(key, SHAPES[name], jnp.float32, 0.005, 0.015)
    return drawn


def matmul(a, w):
    return jnp.dot(a, w, preferred_element_type=jnp.float32).astype(jnp.bfloat16)


def normed(h):
    wide = h.astype(jnp.float32)
    scale = lax.rsqrt(jnp.mean(wide**2, -1, keepdims=True) + 1e-6)
    return (wide * scale).astype(jnp.bfloat16)


def layer(h, w):
    a = normed(h)
    gate = jnp.dot(a, w["w_gate"], preferred_element_type=jnp.float32)
    up = jnp.dot(a, w["w_up"], preferred_element_type=jnp.float32)
    return h + matmul((jax.nn.silu(gate) * up).astype(jnp.bfloat16), w["w_down"])


def adamw(w, m, v, g):
    m = 0.9 * m + 0.1 * g
    v = 0.95 * v + 0.05 * g * g
    step = m * lax.rsqrt(v + 1e-8) + 0.1 * w
    return (w - 0.02 * step).astype(jnp.bfloat16), m, v


def clipped(gradients, sum_of_squares, count):
    factor = jnp.minimum(1.0, 0.5 * lax.rsqrt(sum_of_squares / count + 1e-30))
    return [g * factor for g in gradients]


def stack(weights, h):
    return lax.scan(lambda h, w: (layer(h, w), None), h, weights)[0]


def reference(x, dy, w_gate, w_up, w_down, m_w_gate, m_w_up, m_w_down, v_w_gate, v_w_up, v_w_down):
    weights = dict(zip(NAMES, (w_gate, w_up, w_down), strict=True))

    def take(so_far, sequence):
        h, by_y = sequence
        _, back = jax.vjp(lambda w: stack(w, h), weights)
        return jax.tree.map(lambda total, term: total + term.astype(jnp.float32), so_far, back(by_y)[0]), None

    none_yet = {name: jnp.zeros(w.shape, jnp.float32) for name, w in weights.items()}
    by_weights, _ = lax.scan(take, none_yet, (x, dy))
    gradients = [by_weights[name].astype(jnp.bfloat16).astype(jnp.float32) for name in NAMES]
    gradients = clipped(gradients, sum(jnp.sum(g * g) for g in gradients), sum(g.size for g in gradients))
    new = [
        adamw(w.astype(jnp.float32), m, v, g)
        for w, m, v, g in zip((w_gate, w_up, w_down), (m_w_gate, m_w_up, m_w_down), (v_w_gate, v_w_up, v_w_down), gradients, strict=True)
    ]
    return tuple(one[which] for which in range(3) for one in new)
```

```python
import functools

import jax
import jax.numpy as jnp
from jax import lax
from jax.experimental import pallas as pl
from jax.experimental.pallas import tpu as pltpu
from jax.sharding import PartitionSpec as P

MESH = pl.DeviceIdType.MESH
F32, BF16 = jnp.float32, jnp.bfloat16
SHARE = 32
TILE = 512


def dot(a, b):
    return jnp.dot(a, b, preferred_element_type=F32)


def kernel(n, steps, x_ref, dy_ref, own, g_ref, sq_ref, h, by, byt, a0, a0t, a1, a1t, acc, w, wgut, wdt, part, ring, dgu, ddt, sq, ag_send, ag_recv,
           swap_send, swap_recv, own_sem, in_sem, rs_send, rs_recv, sq_send, sq_recv):
    me, rep = lax.axis_index("dp"), lax.axis_index("rep")
    core = lax.rem(rep, 2)
    sgn = 1 - 2 * core
    tokens, d = h.shape
    tiles = tokens // TILE
    rows_gu = own.shape[1] - SHARE
    width = SHARE * n
    half_rows = own.shape[1] // 2
    half = pl.ds(pl.multiple_of(core * half_rows, 16), half_rows)
    chunks = 2 * steps
    far = n // 2
    slots = ring.shape[0]

    def at(k):
        return lax.rem(k + 2 * n, n)

    def tile(t):
        return pl.ds(pl.multiple_of(t * TILE, TILE), TILE)

    right, left = at(me + sgn), at(me - sgn)
    partner = {"rep": rep + sgn}

    def fetch(t):
        return (
            pltpu.make_async_copy(x_ref.at[tile(t)], h.at[tile(t)], in_sem.at[0, t]),
            pltpu.make_async_copy(dy_ref.at[tile(t)], by.at[tile(t)], in_sem.at[1, t]),
        )

    for t in range(tiles):
        for c in fetch(t):
            c.start()
    own_copy = pltpu.make_async_copy(own.at[:, half], w.at[:, me, half], own_sem)
    own_copy.start()

    barrier = pltpu.get_barrier_semaphore()
    for k in range(1, n):
        pl.semaphore_signal(barrier, inc=1, device_id={"dp": at(me + k)}, device_id_type=MESH)
    pl.semaphore_signal(barrier, inc=1, device_id=partner, device_id_type=MESH)
    pl.semaphore_wait(barrier, n)

    def ag(u, j, long):
        src = at(me - sgn * j) if long else at(me + sgn * j)
        idx = j if long else far + j
        ref = own.at[u, half] if j == 0 else w.at[u, src, half]
        return pltpu.make_async_remote_copy(
            ref, w.at[u, src, half], ag_send.at[u, idx], ag_recv.at[u, idx], device_id={"dp": right if long else left}, device_id_type=MESH
        )

    def ag_arrived(u, j, long):
        src = at(me - sgn * (j + 1)) if long else at(me + sgn * (j + 1))
        idx = j if long else far + j
        ref = w.at[u, src, half]
        pltpu.make_async_remote_copy(
            ref, ref, ag_send.at[u, idx], ag_recv.at[u, idx], device_id={"dp": left if long else right}, device_id_type=MESH
        ).wait_recv()

    def swap(u):
        ref = w.at[u, :, half]
        return pltpu.make_async_remote_copy(ref, ref, swap_send.at[u], swap_recv.at[u], device_id=partner, device_id_type=MESH)

    def ready(u):
        other = pl.ds(pl.multiple_of((1 - core) * half_rows, 16), half_rows)
        ref = w.at[u, :, other]
        pltpu.make_async_remote_copy(ref, ref, swap_send.at[u], swap_recv.at[u], device_id=partner, device_id_type=MESH).wait_recv()

    def when(cond, f):
        if isinstance(cond, bool):
            if cond:
                f()
        else:
            pl.when(cond)(f)

    def both(a, b):
        return (a and b) if isinstance(a, bool) else jnp.logical_and(a, b)

    def stage(i):
        for j in range(far, -1, -1):
            u = i - j

            def hop(u=u, j=j):
                if j > 0:
                    ag_arrived(u, j - 1, True)
                if 0 < j < far:
                    ag_arrived(u, j - 1, False)
                if j < far:
                    ag(u, j, True).start()
                if j < far - 1:
                    ag(u, j, False).start()
                if j == far:
                    if isinstance(u, int):
                        if u == 0:
                            own_copy.wait()
                    swap(u).start()

            when(both(u >= 0, u < chunks), hop)

    def owner(j, long):
        return at(me + sgn * (far - j)) if long else at(me - sgn * (far - 1 - j))

    def rs(q, j, long):
        r, idx = lax.rem(q, slots), j if long else far + j
        src = part.at[lax.rem(q, 3), owner(j, long)] if j == 0 else ring.at[r, idx - 1]
        return pltpu.make_async_remote_copy(
            src, ring.at[r, idx], rs_send.at[r, idx], rs_recv.at[r, idx], device_id={"dp": right if long else left}, device_id_type=MESH
        )

    def rs_arrived(q, j, long):
        r, idx = lax.rem(q, slots), j if long else far + j
        ref = ring.at[r, idx]
        pltpu.make_async_remote_copy(
            ref, ref, rs_send.at[r, idx], rs_recv.at[r, idx], device_id={"dp": left if long else right}, device_id_type=MESH
        ).wait_recv()

    def rs_hop(q, j):
        r = lax.rem(q, slots)
        ways = [True] + [False] * (j < far - 1)
        for long in ways:
            if j > 0:
                rs_arrived(q, j - 1, long)
                idx = j - 1 if long else far + j - 1
                mine = part[lax.rem(q, 3), owner(j, long)].astype(F32)
                ring[r, idx] = (ring[r, idx].astype(F32) + mine).astype(BF16)
        for long in ways:
            rs(q, j, long).start()

    def rs_last(q):
        rs_arrived(q, far - 1, True)
        rs_arrived(q, far - 2, False)
        r = lax.rem(q, slots)
        total = part[lax.rem(q, 3), me].astype(F32) + ring[r, far - 1].astype(F32) + ring[r, 2 * far - 2].astype(F32)
        total = total.astype(BF16)
        g_ref[lax.rem(q + steps, chunks)] = total
        wide = total.astype(F32)
        wide = wide * wide
        sq[...] += jnp.sum(wide.reshape(-1, 8, wide.shape[-1]), axis=0)

    def rs_sent(q):
        for j in range(far):
            rs(q, j, True).wait_send()
        for j in range(far - 1):
            rs(q, j, False).wait_send()

    def rs_middle(q):
        when(both(q >= 2, q < chunks + 2), lambda: rs_hop(q - 2, 3))
        when(both(q >= 1, q < chunks + 1), lambda: rs_hop(q - 1, 1))

    def rs_end(q):
        when(both(q >= 2, q < chunks + 2), lambda: rs_last(q - 2))
        when(both(q >= 1, q < chunks + 1), lambda: rs_hop(q - 1, 2))
        when(both(q >= 0, q < chunks), lambda: rs_hop(q, 0))

    def scale_of(wide):
        return lax.rsqrt(jnp.mean(wide * wide, -1, keepdims=True) + 1e-6)

    def norm_tile(t, src, a, at_):
        wide = src[tile(t)].astype(F32)
        out = (wide * scale_of(wide)).astype(BF16)
        a[tile(t)] = out
        at_[:, tile(t)] = out.T

    def w_gu(u):
        return w[u, :, :rows_gu, :].reshape(n * rows_gu, 2 * width)

    def w_d(u):
        return w[u, :, rows_gu:, :].reshape(width, d)

    sq[...] = jnp.zeros_like(sq)
    stage(0)

    def start_tile(t):
        for c in fetch(t):
            c.wait()
        norm_tile(t, h, a0, a0t)
        byt[:, tile(t)] = by[tile(t)].T

    for i in range(1, far + 1):
        pl.loop(tiles * (i - 1) // far, tiles * i // far)(start_tile)
        stage(i)

    acc[...] = jnp.zeros_like(acc)

    @pl.loop(0, steps)
    def _(s):
        ready(s)

        def forward_tile(t):
            gu = dot(a0[tile(t)], w_gu(s))
            gate, up = gu[:, :width], gu[:, width:]
            act = gate * (0.5 * jnp.tanh(0.5 * gate) + 0.5) * up
            acc[tile(t)] += dot(act.astype(BF16), w_d(s))

        @pl.loop(0, 2)
        def _(part_):
            pl.loop(part_ * (tiles // 2), (part_ + 1) * (tiles // 2))(forward_tile)
            pl.when(part_ == 0)(lambda: stage(s + far + 1))

    @pl.loop(0, tiles)
    def _(t):
        h[tile(t)] = h[tile(t)] + acc[tile(t)].astype(BF16)
        norm_tile(t, h, a1, a1t)

    def backward(first, a, a_t, whole):
        base = steps if whole else 0
        if whole:
            acc[...] = jnp.zeros_like(acc)

        @pl.loop(0, steps)
        def _(s):
            q, u = first + s, base + s
            if whole:
                ready(u)
                wgut[...] = w_gu(u).T
            wdt[...] = w_d(u).T
            dgu[...] = jnp.zeros_like(dgu)
            ddt[...] = jnp.zeros_like(ddt)

            def backward_tile(t):
                gu = dot(a[tile(t)], w_gu(u))
                dact = dot(by[tile(t)], wdt[...]).astype(BF16).astype(F32)
                gate, up = gu[:, :width], gu[:, width:]
                s_ = 0.5 * jnp.tanh(0.5 * gate) + 0.5
                silu = gate * s_
                act = (silu * up).astype(BF16)
                dup = (dact * silu).astype(BF16)
                dgate = (dact * up * (s_ + silu * (1.0 - s_))).astype(BF16)
                both_ = jnp.concatenate([dgate, dup], axis=1)
                dgu[...] += dot(a_t[:, tile(t)], both_)
                ddt[...] += dot(byt[:, tile(t)], act)
                if whole:
                    acc[tile(t)] += dot(both_, wgut[...])

            @pl.loop(0, 2)
            def _(part_):
                pl.loop(part_ * (tiles // 2), (part_ + 1) * (tiles // 2))(backward_tile)

                @pl.when(part_ == 0)
                def _():
                    if whole:
                        stage(u + far + 1)
                    rs_middle(q)

            when(q >= 3, lambda: rs_sent(q - 3))
            p = lax.rem(q, 3)
            part[p, :, :rows_gu, :] = dgu[...].astype(BF16).reshape(n, rows_gu, 2 * width)
            part[p, :, rows_gu:, :] = ddt[...].T.astype(BF16).reshape(n, SHARE, d)
            rs_end(q)

    backward(0, a1, a1t, True)

    @pl.loop(0, tiles)
    def _(t):
        wide = h[tile(t)].astype(F32)
        scale = scale_of(wide)
        ct = acc[tile(t)].astype(BF16).astype(F32)
        back = scale * ct - wide * (scale * scale * scale) * jnp.mean(ct * wide, -1, keepdims=True)
        new = by[tile(t)] + back.astype(BF16)
        by[tile(t)] = new
        byt[:, tile(t)] = new.T

    backward(steps, a0, a0t, False)

    for q in (chunks, chunks + 1):
        rs_middle(q)
        rs_sent(q - 3)
        rs_end(q)
    rs_sent(chunks - 1)

    sq_ref[me] = jnp.sum(sq[...].reshape(8, -1, 128), axis=1)
    for k in range(1, n):
        pltpu.make_async_remote_copy(
            sq_ref.at[me], sq_ref.at[me], sq_send.at[k], sq_recv.at[k], device_id={"dp": at(me + k)}, device_id_type=MESH
        ).start()
    for k in range(1, n):
        ref = sq_ref.at[at(me - k)]
        c = pltpu.make_async_remote_copy(ref, ref, sq_send.at[k], sq_recv.at[k], device_id={"dp": at(me + k)}, device_id_type=MESH)
        c.wait_recv()
    for k in range(1, n):
        ref = sq_ref.at[me]
        pltpu.make_async_remote_copy(ref, ref, sq_send.at[k], sq_recv.at[k], device_id={"dp": at(me + k)}, device_id_type=MESH).wait_send()

    @pl.loop(0, chunks)
    def _(u):
        for j in range(far):
            ag(u, j, True).wait_send()
        for j in range(far - 1):
            ag(u, j, False).wait_send()
        swap(u).wait_send()


def grouped(n, share):
    steps = -(-share // SHARE)
    f = jnp.arange(n * share, dtype=jnp.int32)
    k, r = f // share, f % share
    to = (r // SHARE) * (n * SHARE) + k * SHARE + r % SHARE
    return (to[:, None] == jnp.arange(n * steps * SHARE, dtype=jnp.int32)[None, :]).astype(BF16), steps


def adamw(w, m, v, g):
    m = 0.9 * m + 0.1 * g
    v = 0.95 * v + 0.05 * g * g
    step = m * lax.rsqrt(v + 1e-8) + 0.1 * w
    return (w - 0.02 * step).astype(BF16), m, v


def clipped(gradients, sum_of_squares, count):
    factor = jnp.minimum(1.0, 0.5 * lax.rsqrt(sum_of_squares / count + 1e-30))
    return [g * factor for g in gradients]


def solution(mesh):
    n = mesh.shape["dp"]

    def step(x, dy, *arrays):
        weights, m, v = (arrays[i : i + 3] for i in (0, 3, 6))
        w_gate, w_up, w_down = weights
        layers, rows, _ = w_gate.shape
        share, d = w_down.shape[1:]
        tokens = x.shape[1]
        onehot, steps = grouped(n, share)
        width = n * SHARE
        chunks = layers * steps

        def spread(w):
            w = dot(w.reshape(layers * rows, -1), onehot).astype(BF16)
            return w.reshape(layers, rows, steps, width).transpose(0, 2, 1, 3)

        down = jnp.pad(w_down, ((0, 0), (0, steps * SHARE - share), (0, 0))).reshape(layers, steps, SHARE, d)
        own = jnp.concatenate([jnp.concatenate([spread(w_gate), spread(w_up)], -1), down], 2).reshape(chunks, rows + SHARE, d)

        slots, hops = 4, n - 1
        dma = pltpu.SemaphoreType.DMA
        g, squares = pl.pallas_call(
            functools.partial(kernel, n, steps),
            out_shape=(jax.ShapeDtypeStruct((chunks, rows + SHARE, d), BF16), jax.ShapeDtypeStruct((n, 8, 128), F32)),
            in_specs=[pl.BlockSpec(memory_space=pl.ANY)] * 2 + [pl.BlockSpec(memory_space=pltpu.VMEM)],
            out_specs=(pl.BlockSpec(memory_space=pltpu.VMEM),) * 2,
            scratch_shapes=[
                pltpu.VMEM((tokens, d), BF16),
                pltpu.VMEM((tokens, d), BF16),
                pltpu.VMEM((d, tokens), BF16),
                pltpu.VMEM((tokens, d), BF16),
                pltpu.VMEM((d, tokens), BF16),
                pltpu.VMEM((tokens, d), BF16),
                pltpu.VMEM((d, tokens), BF16),
                pltpu.VMEM((tokens, d), F32),
                pltpu.VMEM((chunks, n, rows + SHARE, d), BF16),
                pltpu.VMEM((2 * width, d), BF16),
                pltpu.VMEM((d, width), BF16),
                pltpu.VMEM((3, n, rows + SHARE, d), BF16),
                pltpu.VMEM((slots, hops, rows + SHARE, d), BF16),
                pltpu.VMEM((d, 2 * width), F32),
                pltpu.VMEM((d, width), F32),
                pltpu.VMEM((8, d), F32),
                dma((chunks, hops)),
                dma((chunks, hops)),
                dma((chunks,)),
                dma((chunks,)),
                dma,
                dma((2, tokens // TILE)),
                dma((slots, hops)),
                dma((slots, hops)),
                dma((n,)),
                dma((n,)),
            ],
            compiler_params=pltpu.CompilerParams(collective_id=0, has_side_effects=True, vmem_limit_bytes=67043328),
            name="step",
        )(x[0], dy[0], own)

        g = g.reshape(layers, steps, rows + SHARE, d)

        def gathered(part):
            part = part.transpose(0, 2, 1, 3).reshape(layers * rows, steps * width)
            return lax.dot_general(part, onehot, (((1,), (1,)), ((), ())), preferred_element_type=F32).reshape(layers, rows, -1)

        gradients = [
            gathered(g[:, :, :rows, :width]),
            gathered(g[:, :, :rows, width:]),
            g[:, :, rows:].reshape(layers, steps * SHARE, d)[:, :share].astype(F32),
        ]
        gradients = clipped(gradients, jnp.sum(squares), n * sum(one.size for one in gradients))
        new = [adamw(w.astype(F32), m, v, g) for w, m, v, g in zip(weights, m, v, gradients, strict=True)]
        return tuple(one[which] for which in range(3) for one in new)

    states, cut = P(("rep", "dp"), None, None), P(None, "dp", None)
    return jax.shard_map(
        step,
        mesh=mesh,
        in_specs=(states, states) + (cut,) * 9,
        out_specs=(P("rep", "dp", None),) * 9,
        check_vma=False,
    )
```

```python
import functools

import jax
import jax.numpy as jnp
from jax import lax
from jax.experimental import pallas as pl
from jax.experimental.pallas import tpu as pltpu
from jax.sharding import PartitionSpec as P

MESH = pl.DeviceIdType.MESH
F32, BF16 = jnp.float32, jnp.bfloat16
SHARE = 32
TILE = 512
BIG = 2048


def dot(a, b):
    return jnp.dot(a, b, preferred_element_type=F32)


def dot_nt(a, b):
    return lax.dot_general(a, b, (((1,), (1,)), ((), ())), preferred_element_type=F32)


def kernel(n, steps, x_ref, dy_ref, wg_ref, wu_ref, wd_ref, gg_ref, gu_ref, gd_ref, f_ref, h, by, byt, a0, a0t, a1, a1t, acc, own, w, part, ring, dgu,
           ddt, sq, sq_all, ag_send, ag_recv, swap_send, swap_recv, own_sem, in_sem, rs_send, rs_recv, sq_send, sq_recv):
    me, rep = lax.axis_index("dp"), lax.axis_index("rep")
    core = lax.rem(rep, 2)
    sgn = 1 - 2 * core
    tokens, d = h.shape
    tiles = tokens // TILE
    rows_gu = own.shape[1] - SHARE
    width = SHARE * n
    half_rows = own.shape[1] // 2
    half = pl.ds(pl.multiple_of(core * half_rows, 16), half_rows)
    chunks = 2 * steps
    far = n // 2
    slots = ring.shape[0]

    def at(k):
        return lax.rem(k + 2 * n, n)

    def tile(t):
        return pl.ds(pl.multiple_of(t * TILE, TILE), TILE)

    def cut_by(size):
        return tokens // size, lambda t: pl.ds(pl.multiple_of(t * size, size), size)

    right, left = at(me + sgn), at(me - sgn)
    partner = {"rep": rep + sgn}

    def fetch(t):
        return (
            pltpu.make_async_copy(x_ref.at[tile(t)], h.at[tile(t)], in_sem.at[0, t]),
            pltpu.make_async_copy(dy_ref.at[tile(t)], by.at[tile(t)], in_sem.at[1, t]),
        )

    for t in range(tiles):
        for c in fetch(t):
            c.start()

    barrier = pltpu.get_barrier_semaphore()
    for k in range(1, n):
        pl.semaphore_signal(barrier, inc=1, device_id={"dp": at(me + k)}, device_id_type=MESH)
    pl.semaphore_signal(barrier, inc=1, device_id=partner, device_id_type=MESH)

    layers, rows, hidden = wg_ref.shape
    share = wd_ref.shape[1]
    both_w = jnp.concatenate([wg_ref[...].reshape(layers * rows, hidden), wu_ref[...].reshape(layers * rows, hidden)], 0)
    place = lax.broadcasted_iota(jnp.int32, (1, width), 1)
    unit = lax.broadcasted_iota(jnp.int32, (hidden, width), 0)
    for s in range(steps):
        size = min(SHARE, share - s * SHARE)
        wanted = jnp.where(place < size * n, place // size * share + s * SHARE + place % size, -1)
        pick = jnp.where(unit == wanted, 1.0, 0.0).astype(BF16)
        cut = dot(both_w, pick).astype(BF16).reshape(2, layers, rows, width)
        for l in range(layers):
            block, down = own.at[l * steps + s], wd_ref[l, s * SHARE : s * SHARE + size]
            if size == SHARE:
                block[:rows, :width] = cut[0, l]
                block[:rows, width:] = cut[1, l]
                block[rows:] = down
            else:
                block[:rows, : width // 2] = cut[0, l, :, : width // 2]
                block[:rows, width // 2 : width] = cut[1, l, :, : width // 2]
                block[rows : rows + size, :width] = down[:, :width]
                block[rows + size :, :width] = down[:, width:]
                block[:, width:] = jnp.zeros((rows + SHARE, width), BF16)
    pl.semaphore_wait(barrier, n)
    own_copy = pltpu.make_async_copy(own.at[:, half], w.at[:, me, half], own_sem)
    own_copy.start()

    def sized(c, f):
        if isinstance(c, int):
            f(c % steps == steps - 1)
        else:
            pl.when(lax.rem(c, steps) != steps - 1)(lambda: f(False))
            pl.when(lax.rem(c, steps) == steps - 1)(lambda: f(True))

    def lanes(narrow):
        return pl.ds(0, width if narrow else d)

    def ag(u, j, long, narrow):
        src = at(me - sgn * j) if long else at(me + sgn * j)
        idx = j if long else far + j
        ref = own.at[u, half, lanes(narrow)] if j == 0 else w.at[u, src, half, lanes(narrow)]
        to = w.at[u, src, half, lanes(narrow)]
        return pltpu.make_async_remote_copy(
            ref, to, ag_send.at[u, idx], ag_recv.at[u, idx], device_id={"dp": right if long else left}, device_id_type=MESH
        )

    def ag_arrived(u, j, long, narrow):
        src = at(me - sgn * (j + 1)) if long else at(me + sgn * (j + 1))
        idx = j if long else far + j
        ref = w.at[u, src, half, lanes(narrow)]
        pltpu.make_async_remote_copy(
            ref, ref, ag_send.at[u, idx], ag_recv.at[u, idx], device_id={"dp": left if long else right}, device_id_type=MESH
        ).wait_recv()

    def swap(u, narrow):
        ref = w.at[u, :, half, lanes(narrow)]
        return pltpu.make_async_remote_copy(ref, ref, swap_send.at[u], swap_recv.at[u], device_id=partner, device_id_type=MESH)

    def ready(u, narrow):
        other = pl.ds(pl.multiple_of((1 - core) * half_rows, 16), half_rows)
        ref = w.at[u, :, other, lanes(narrow)]
        pltpu.make_async_remote_copy(ref, ref, swap_send.at[u], swap_recv.at[u], device_id=partner, device_id_type=MESH).wait_recv()

    def when(cond, f):
        if isinstance(cond, bool):
            if cond:
                f()
        else:
            pl.when(cond)(f)

    def both(a, b):
        return (a and b) if isinstance(a, bool) else jnp.logical_and(a, b)

    def stage(i, odd):
        for j in range(far, -1, -1):
            if j % 2 != odd:
                continue
            u = i + (odd - 3 * j) // 2

            def hop(narrow, u=u, j=j):
                if j > 0:
                    ag_arrived(u, j - 1, True, narrow)
                if 0 < j < far:
                    ag_arrived(u, j - 1, False, narrow)
                if j < far:
                    ag(u, j, True, narrow).start()
                if j < far - 1:
                    ag(u, j, False, narrow).start()
                if j == far:
                    if isinstance(u, int):
                        if u == 0:
                            own_copy.wait()
                    swap(u, narrow).start()

            when(both(u >= 0, u < chunks), lambda u=u, hop=hop: sized(u, hop))

    def owner(j, long):
        return at(me + sgn * (far - j)) if long else at(me - sgn * (far - 1 - j))

    def rs(q, j, long, narrow):
        r, idx = lax.rem(q, slots), j if long else far + j
        src = part.at[lax.rem(q, 3), owner(j, long)] if j == 0 else ring.at[r, idx - 1]
        return pltpu.make_async_remote_copy(
            src.at[:, lanes(narrow)],
            ring.at[r, idx, :, lanes(narrow)],
            rs_send.at[r, idx],
            rs_recv.at[r, idx],
            device_id={"dp": right if long else left},
            device_id_type=MESH,
        )

    def rs_arrived(q, j, long, narrow):
        r, idx = lax.rem(q, slots), j if long else far + j
        ref = ring.at[r, idx, :, lanes(narrow)]
        pltpu.make_async_remote_copy(
            ref, ref, rs_send.at[r, idx], rs_recv.at[r, idx], device_id={"dp": left if long else right}, device_id_type=MESH
        ).wait_recv()

    def rs_hop(q, j, narrow):
        r = lax.rem(q, slots)
        ways = [True] + [False] * (j < far - 1)
        for long in ways:
            if j > 0:
                rs_arrived(q, j - 1, long, narrow)
                idx = j - 1 if long else far + j - 1
                mine = part[lax.rem(q, 3), owner(j, long), :, lanes(narrow)].astype(F32)
                ring[r, idx, :, lanes(narrow)] = (ring[r, idx, :, lanes(narrow)].astype(F32) + mine).astype(BF16)
        for long in ways:
            rs(q, j, long, narrow).start()

    def rs_last(q, narrow):
        rs_arrived(q, far - 1, True, narrow)
        rs_arrived(q, far - 2, False, narrow)
        r, cols = lax.rem(q, slots), lanes(narrow)
        total = part[lax.rem(q, 3), me, :, cols].astype(F32) + ring[r, far - 1, :, cols].astype(F32) + ring[r, 2 * far - 2, :, cols].astype(F32)
        total = total.astype(BF16)
        u = lax.rem(q + steps, chunks)
        l = lax.div(u, steps)
        if narrow:
            at_, end = (steps - 1) * width, (steps - 1) * SHARE
            gg_ref[l, :, at_:] = total[:rows_gu, : width // 2]
            gu_ref[l, :, at_:] = total[:rows_gu, width // 2 :]
            gd_ref[l, end:, :width] = total[rows_gu : rows_gu + SHARE // 2]
            gd_ref[l, end:, width:] = total[rows_gu + SHARE // 2 :]
        else:
            s = lax.rem(u, steps)
            gg_ref[l, :, pl.ds(pl.multiple_of(s * width, width), width)] = total[:rows_gu, :width]
            gu_ref[l, :, pl.ds(pl.multiple_of(s * width, width), width)] = total[:rows_gu, width:]
            gd_ref[l, pl.ds(pl.multiple_of(s * SHARE, SHARE), SHARE)] = total[rows_gu:]
        wide = total.astype(F32)
        wide = wide * wide
        sq[:, cols] += jnp.sum(wide.reshape(-1, 8, wide.shape[-1]), axis=0)
        for j in range(far):
            rs(q, j, True, narrow).wait_send()
        for j in range(far - 1):
            rs(q, j, False, narrow).wait_send()

    def rs_slot(q, slot):
        j = 4 - slot
        c = q - j
        when(both(c >= 0, c < chunks), lambda: sized(c, lambda narrow: rs_hop(c, j, narrow)))

    def rs_end(q):
        c = q - 3
        when(both(c >= 0, c < chunks), lambda: sized(c, lambda narrow: rs_last(c, narrow)))

    def scale_of(wide):
        return lax.rsqrt(jnp.mean(wide * wide, -1, keepdims=True) + 1e-6)

    def norm_tile(t, src, a, at_):
        wide = src[tile(t)].astype(F32)
        out = (wide * scale_of(wide)).astype(BF16)
        a[tile(t)] = out
        at_[:, tile(t)] = out.T

    def w_gu(u, narrow):
        return w[u, :, :rows_gu, lanes(narrow)].reshape(n * rows_gu, -1)

    def w_d(u, narrow):
        if not narrow:
            return w[u, :, rows_gu:, :].reshape(width, d)
        mid = rows_gu + SHARE // 2
        return jnp.concatenate([w[u, :, rows_gu:mid, :width].reshape(-1, width), w[u, :, mid:, :width].reshape(-1, width)], 1)

    sq[...] = jnp.zeros_like(sq)
    ahead = 3 * far // 2

    def start_tile(t):
        for c in fetch(t):
            c.wait()
        norm_tile(t, h, a0, a0t)
        byt[:, tile(t)] = by[tile(t)].T

    for i in range(ahead + 1):
        stage(i, 0)
        if 1 <= i <= far:
            pl.loop(tiles * (i - 1) // far, tiles * i // far)(start_tile)
        stage(i, 1)

    acc[...] = jnp.zeros_like(acc)

    def forward(s, narrow):
        ready(s, narrow)
        size = BIG // 2 if narrow else BIG
        count, big = cut_by(size)

        @pl.loop(0, count)
        def _(t):
            gu = dot(a0[big(t)], w_gu(s, narrow))
            units = gu.shape[1] // 2
            gate, up = gu[:, :units], gu[:, units:]
            act = gate * (0.5 * jnp.tanh(0.5 * gate) + 0.5) * up
            acc[big(t)] += dot(act.astype(BF16), w_d(s, narrow))
            pl.when(t == count // 2 - 1)(lambda: stage(s + ahead + 1, 0))
            pl.when(t == count - 1)(lambda: stage(s + ahead + 1, 1))

    @pl.loop(0, steps - 1)
    def _(s):
        forward(s, False)

    forward(steps - 1, True)

    @pl.loop(0, tiles)
    def _(t):
        h[tile(t)] = h[tile(t)] + acc[tile(t)].astype(BF16)
        norm_tile(t, h, a1, a1t)

    def backward(first, a, a_t, whole):
        base = steps if whole else 0
        if whole:
            acc[...] = jnp.zeros_like(acc)

        dgu[...] = jnp.zeros_like(dgu)
        ddt[...] = jnp.zeros_like(ddt)

        def chunk(s, narrow):
            q, u = first + s, base + s
            if whole:
                ready(u, narrow)
            count, big = cut_by(BIG // 2 if narrow else BIG)
            units = width // 2 if narrow else width

            @pl.loop(0, count)
            def _(t):
                gu = dot(a[big(t)], w_gu(u, narrow))
                dact = dot_nt(by[big(t)], w_d(u, narrow)).astype(BF16).astype(F32)
                gate, up = gu[:, :units], gu[:, units:]
                s_ = 0.5 * jnp.tanh(0.5 * gate) + 0.5
                silu = gate * s_
                act = (silu * up).astype(BF16)
                dup = (dact * silu).astype(BF16)
                dgate = (dact * up * (s_ + silu * (1.0 - s_))).astype(BF16)
                both_ = jnp.concatenate([dgate, dup], axis=1)
                dgu[:, : 2 * units] += dot(a_t[:, big(t)], both_)
                ddt[:, :units] += dot(byt[:, big(t)], act)
                if whole:
                    acc[big(t)] += dot_nt(both_, w_gu(u, narrow))
                for slot in (1, 2, 3):

                    @pl.when(t == -(-slot * count // 4) - 1)
                    def _():
                        if whole and slot != 2:
                            for odd in (0, 1):
                                stage(base + ahead + 1 + 2 * s + slot // 2, odd)
                        rs_slot(q, slot)

            rs_end(q)
            p = lax.rem(q, 3)
            part[p, :, :rows_gu, lanes(narrow)] = dgu[:, : 2 * units].astype(BF16).reshape(n, rows_gu, 2 * units)
            down = ddt[:, :units].T.astype(BF16)
            if narrow:
                mid = rows_gu + SHARE // 2
                part[p, :, rows_gu:mid, :width] = down[:, :width].reshape(n, SHARE // 2, width)
                part[p, :, mid:, :width] = down[:, width:].reshape(n, SHARE // 2, width)
            else:
                part[p, :, rows_gu:, :] = down.reshape(n, SHARE, d)
                dgu[...] = jnp.zeros_like(dgu)
                ddt[...] = jnp.zeros_like(ddt)
            rs_hop(q, 0, narrow)

        @pl.loop(0, steps - 1)
        def _(s):
            chunk(s, False)

        chunk(steps - 1, True)

    backward(0, a1, a1t, True)

    @pl.loop(0, tiles)
    def _(t):
        wide = h[tile(t)].astype(F32)
        scale = scale_of(wide)
        ct = acc[tile(t)].astype(BF16).astype(F32)
        back = scale * ct - wide * (scale * scale * scale) * jnp.mean(ct * wide, -1, keepdims=True)
        new = by[tile(t)] + back.astype(BF16)
        by[tile(t)] = new
        byt[:, tile(t)] = new.T

    backward(steps, a0, a0t, False)

    for q in range(chunks, chunks + 3):
        for slot in (1, 2, 3):
            rs_slot(q, slot)
        rs_end(q)

    sq_all[me] = jnp.sum(sq[...].reshape(8, -1, 128), axis=1)
    for k in range(1, n):
        pltpu.make_async_remote_copy(
            sq_all.at[me], sq_all.at[me], sq_send.at[k], sq_recv.at[k], device_id={"dp": at(me + k)}, device_id_type=MESH
        ).start()
    for k in range(1, n):
        ref = sq_all.at[at(me - k)]
        c = pltpu.make_async_remote_copy(ref, ref, sq_send.at[k], sq_recv.at[k], device_id={"dp": at(me + k)}, device_id_type=MESH)
        c.wait_recv()
    for k in range(1, n):
        ref = sq_all.at[me]
        pltpu.make_async_remote_copy(ref, ref, sq_send.at[k], sq_recv.at[k], device_id={"dp": at(me + k)}, device_id_type=MESH).wait_send()

    factor = jnp.minimum(1.0, 0.5 * lax.rsqrt(jnp.sum(sq_all[...]) / (n * layers * (2 * rows * hidden + share * d)) + 1e-30))
    f_ref[...] = jnp.full(f_ref.shape, factor)

    def sent(narrow, u):
        for j in range(far):
            ag(u, j, True, narrow).wait_send()
        for j in range(far - 1):
            ag(u, j, False, narrow).wait_send()
        swap(u, narrow).wait_send()

    @pl.loop(0, chunks)
    def _(u):
        sized(u, lambda narrow: sent(narrow, u))


def grouped(n, share):
    steps = -(-share // SHARE)
    f = jnp.arange(n * share, dtype=jnp.int32)
    k, s, r = f // share, f % share // SHARE, f % share % SHARE
    to = s * (n * SHARE) + k * jnp.minimum(SHARE, share - s * SHARE) + r
    return (to[:, None] == f[None, :]).astype(BF16), steps


def adamw(w, m, v, g):
    m = 0.9 * m + 0.1 * g
    v = 0.95 * v + 0.05 * g * g
    step = m * lax.rsqrt(v + 1e-8) + 0.1 * w
    return (w - 0.02 * step).astype(BF16), m, v


def solution(mesh):
    n = mesh.shape["dp"]

    def step(x, dy, *arrays):
        weights, m, v = (arrays[i : i + 3] for i in (0, 3, 6))
        w_gate, w_up, w_down = weights
        layers, rows, _ = w_gate.shape
        share, d = w_down.shape[1:]
        tokens = x.shape[1]
        onehot, steps = grouped(n, share)
        width = n * SHARE
        chunks = layers * steps

        slots, hops = 5, n - 1
        dma = pltpu.SemaphoreType.DMA
        g_gate, g_up, g_down, factor = pl.pallas_call(
            functools.partial(kernel, n, steps),
            out_shape=(
                jax.ShapeDtypeStruct((layers, rows, n * share), BF16),
                jax.ShapeDtypeStruct((layers, rows, n * share), BF16),
                jax.ShapeDtypeStruct((layers, share, d), BF16),
                jax.ShapeDtypeStruct((8, 128), F32),
            ),
            in_specs=[pl.BlockSpec(memory_space=pl.ANY)] * 2 + [pl.BlockSpec(memory_space=pltpu.VMEM)] * 3,
            out_specs=(pl.BlockSpec(memory_space=pltpu.VMEM),) * 4,
            scratch_shapes=[
                pltpu.VMEM((tokens, d), BF16),
                pltpu.VMEM((tokens, d), BF16),
                pltpu.VMEM((d, tokens), BF16),
                pltpu.VMEM((tokens, d), BF16),
                pltpu.VMEM((d, tokens), BF16),
                pltpu.VMEM((tokens, d), BF16),
                pltpu.VMEM((d, tokens), BF16),
                pltpu.VMEM((tokens, d), F32),
                pltpu.VMEM((chunks, rows + SHARE, d), BF16),
                pltpu.VMEM((chunks, n, rows + SHARE, d), BF16),
                pltpu.VMEM((3, n, rows + SHARE, d), BF16),
                pltpu.VMEM((slots, hops, rows + SHARE, d), BF16),
                pltpu.VMEM((d, 2 * width), F32),
                pltpu.VMEM((d, width), F32),
                pltpu.VMEM((8, d), F32),
                pltpu.VMEM((n, 8, 128), F32),
                dma((chunks, hops)),
                dma((chunks, hops)),
                dma((chunks,)),
                dma((chunks,)),
                dma,
                dma((2, tokens // TILE)),
                dma((slots, hops)),
                dma((slots, hops)),
                dma((n,)),
                dma((n,)),
            ],
            compiler_params=pltpu.CompilerParams(collective_id=0, has_side_effects=True, vmem_limit_bytes=67043328),
            name="step",
        )(x[0], dy[0], *weights)

        def gathered(part):
            part = part.reshape(layers * rows, n * share)
            return lax.dot_general(part, onehot, (((1,), (1,)), ((), ())), preferred_element_type=F32).reshape(layers, rows, -1)

        factor = factor[0, 0]
        gradients = [factor * g for g in (gathered(g_gate), gathered(g_up), g_down.astype(F32))]
        new = [adamw(w.astype(F32), m, v, g) for w, m, v, g in zip(weights, m, v, gradients, strict=True)]
        return tuple(one[which] for which in range(3) for one in new)

    states, cut = P(("rep", "dp"), None, None), P(None, "dp", None)
    return jax.shard_map(
        step,
        mesh=mesh,
        in_specs=(states, states) + (cut,) * 9,
        out_specs=(P("rep", "dp", None),) * 9,
        check_vma=False,
    )
```

```python
import functools

import jax
import jax.numpy as jnp
from jax import lax
from jax.experimental import pallas as pl
from jax.experimental.pallas import tpu as pltpu
from jax.sharding import PartitionSpec as P

MESH = pl.DeviceIdType.MESH
F32, BF16 = jnp.float32, jnp.bfloat16
SHARE = 32
TILE = 512
BIG = 2048


def dot(a, b):
    return jnp.dot(a, b, preferred_element_type=F32)


def dot_nt(a, b):
    return lax.dot_general(a, b, (((1,), (1,)), ((), ())), preferred_element_type=F32)


def kernel(n, steps, x_ref, dy_ref, wg_ref, wu_ref, wd_ref, gg_ref, gu_ref, gd_ref, f_ref, h, by, byt, a0, a0t, a1, a1t, acc, own, w, part, ring, dgu,
           ddt, sq, sq_all, ag_send, ag_recv, swap_send, swap_recv, own_sem, in_sem, rs_send, rs_recv, sq_send, sq_recv):
    me, rep = lax.axis_index("dp"), lax.axis_index("rep")
    core = lax.rem(rep, 2)
    sgn = 1 - 2 * core
    tokens, d = h.shape
    tiles = tokens // TILE
    rows_gu = own.shape[1] - SHARE
    width = SHARE * n
    half_rows = own.shape[1] // 2
    half = pl.ds(pl.multiple_of(core * half_rows, 16), half_rows)
    chunks = 2 * steps
    far = n // 2
    slots = ring.shape[0]

    def at(k):
        return lax.rem(k + 2 * n, n)

    def tile(t):
        return pl.ds(pl.multiple_of(t * TILE, TILE), TILE)

    def cut_by(size):
        return tokens // size, lambda t: pl.ds(pl.multiple_of(t * size, size), size)

    right, left = at(me + sgn), at(me - sgn)
    partner = {"rep": rep + sgn}

    def fetch(t):
        return (
            pltpu.make_async_copy(x_ref.at[tile(t)], h.at[tile(t)], in_sem.at[0, t]),
            pltpu.make_async_copy(dy_ref.at[tile(t)], by.at[tile(t)], in_sem.at[1, t]),
        )

    for t in range(tiles):
        for c in fetch(t):
            c.start()

    barrier = pltpu.get_barrier_semaphore()
    for k in range(1, n):
        pl.semaphore_signal(barrier, inc=1, device_id={"dp": at(me + k)}, device_id_type=MESH)
    pl.semaphore_signal(barrier, inc=1, device_id=partner, device_id_type=MESH)

    layers, rows, hidden = wg_ref.shape
    share = wd_ref.shape[1]
    both_w = jnp.concatenate([wg_ref[...].reshape(layers * rows, hidden), wu_ref[...].reshape(layers * rows, hidden)], 0)
    place = lax.broadcasted_iota(jnp.int32, (1, width), 1)
    unit = lax.broadcasted_iota(jnp.int32, (hidden, width), 0)
    for s in range(steps):
        size = min(SHARE, share - s * SHARE)
        wanted = jnp.where(place < size * n, place // size * share + s * SHARE + place % size, -1)
        pick = jnp.where(unit == wanted, 1.0, 0.0).astype(BF16)
        cut = dot(both_w, pick).astype(BF16).reshape(2, layers, rows, width)
        for l in range(layers):
            block, down = own.at[l * steps + s], wd_ref[l, s * SHARE : s * SHARE + size]
            if size == SHARE:
                block[:rows, :width] = cut[0, l]
                block[:rows, width:] = cut[1, l]
                block[rows:] = down
            else:
                block[:rows, : width // 2] = cut[0, l, :, : width // 2]
                block[:rows, width // 2 : width] = cut[1, l, :, : width // 2]
                block[rows : rows + size, :width] = down[:, :width]
                block[rows + size :, :width] = down[:, width:]
                block[:, width:] = jnp.zeros((rows + SHARE, width), BF16)
    pl.semaphore_wait(barrier, n)
    own_copy = pltpu.make_async_copy(own.at[:, half], w.at[:, me, half], own_sem)
    own_copy.start()

    def sized(c, f):
        if isinstance(c, int):
            f(c % steps == steps - 1)
        else:
            pl.when(lax.rem(c, steps) != steps - 1)(lambda: f(False))
            pl.when(lax.rem(c, steps) == steps - 1)(lambda: f(True))

    def lanes(narrow):
        return pl.ds(0, width if narrow else d)

    def ag(u, j, long, narrow):
        src = at(me - sgn * j) if long else at(me + sgn * j)
        idx = j if long else far + j
        ref = own.at[u, half, lanes(narrow)] if j == 0 else w.at[u, src, half, lanes(narrow)]
        to = w.at[u, src, half, lanes(narrow)]
        return pltpu.make_async_remote_copy(
            ref, to, ag_send.at[u, idx], ag_recv.at[u, idx], device_id={"dp": right if long else left}, device_id_type=MESH
        )

    def ag_arrived(u, j, long, narrow):
        src = at(me - sgn * (j + 1)) if long else at(me + sgn * (j + 1))
        idx = j if long else far + j
        ref = w.at[u, src, half, lanes(narrow)]
        pltpu.make_async_remote_copy(
            ref, ref, ag_send.at[u, idx], ag_recv.at[u, idx], device_id={"dp": left if long else right}, device_id_type=MESH
        ).wait_recv()

    def swap(u, narrow):
        ref = w.at[u, :, half, lanes(narrow)]
        return pltpu.make_async_remote_copy(ref, ref, swap_send.at[u], swap_recv.at[u], device_id=partner, device_id_type=MESH)

    def ready(u, narrow):
        other = pl.ds(pl.multiple_of((1 - core) * half_rows, 16), half_rows)
        ref = w.at[u, :, other, lanes(narrow)]
        pltpu.make_async_remote_copy(ref, ref, swap_send.at[u], swap_recv.at[u], device_id=partner, device_id_type=MESH).wait_recv()

    def when(cond, f):
        if isinstance(cond, bool):
            if cond:
                f()
        else:
            pl.when(cond)(f)

    def both(a, b):
        return (a and b) if isinstance(a, bool) else jnp.logical_and(a, b)

    def stage(i, odd):
        for j in range(far, -1, -1):
            if j % 2 != odd:
                continue
            u = i + (odd - 3 * j) // 2

            def hop(narrow, u=u, j=j):
                if j > 0:
                    ag_arrived(u, j - 1, True, narrow)
                if 0 < j < far:
                    ag_arrived(u, j - 1, False, narrow)
                if j < far:
                    ag(u, j, True, narrow).start()
                if j < far - 1:
                    ag(u, j, False, narrow).start()
                if j == far:
                    if isinstance(u, int):
                        if u == 0:
                            own_copy.wait()
                    swap(u, narrow).start()

            when(both(u >= 0, u < chunks), lambda u=u, hop=hop: sized(u, hop))

    def owner(j, long):
        return at(me + sgn * (far - j)) if long else at(me - sgn * (far - 1 - j))

    def rs(q, j, long, narrow):
        r, idx = lax.rem(q, slots), j if long else far + j
        src = part.at[lax.rem(q, 3), owner(j, long)] if j == 0 else ring.at[r, idx - 1]
        return pltpu.make_async_remote_copy(
            src.at[:, lanes(narrow)],
            ring.at[r, idx, :, lanes(narrow)],
            rs_send.at[r, idx],
            rs_recv.at[r, idx],
            device_id={"dp": right if long else left},
            device_id_type=MESH,
        )

    def rs_arrived(q, j, long, narrow):
        r, idx = lax.rem(q, slots), j if long else far + j
        ref = ring.at[r, idx, :, lanes(narrow)]
        pltpu.make_async_remote_copy(
            ref, ref, rs_send.at[r, idx], rs_recv.at[r, idx], device_id={"dp": left if long else right}, device_id_type=MESH
        ).wait_recv()

    def rs_hop(q, j, narrow):
        r = lax.rem(q, slots)
        ways = [True] + [False] * (j < far - 1)
        for long in ways:
            if j > 0:
                rs_arrived(q, j - 1, long, narrow)
                idx = j - 1 if long else far + j - 1
                mine = part[lax.rem(q, 3), owner(j, long), :, lanes(narrow)].astype(F32)
                ring[r, idx, :, lanes(narrow)] = (ring[r, idx, :, lanes(narrow)].astype(F32) + mine).astype(BF16)
        for long in ways:
            rs(q, j, long, narrow).start()

    def rs_last(q, narrow):
        rs_arrived(q, far - 1, True, narrow)
        rs_arrived(q, far - 2, False, narrow)
        r, cols = lax.rem(q, slots), lanes(narrow)
        total = part[lax.rem(q, 3), me, :, cols].astype(F32) + ring[r, far - 1, :, cols].astype(F32) + ring[r, 2 * far - 2, :, cols].astype(F32)
        total = total.astype(BF16)
        u = lax.rem(q + steps, chunks)
        l = lax.div(u, steps)
        if narrow:
            at_, end = (steps - 1) * width, (steps - 1) * SHARE
            gg_ref[l, :, at_:] = total[:rows_gu, : width // 2]
            gu_ref[l, :, at_:] = total[:rows_gu, width // 2 :]
            gd_ref[l, end:, :width] = total[rows_gu : rows_gu + SHARE // 2]
            gd_ref[l, end:, width:] = total[rows_gu + SHARE // 2 :]
        else:
            s = lax.rem(u, steps)
            gg_ref[l, :, pl.ds(pl.multiple_of(s * width, width), width)] = total[:rows_gu, :width]
            gu_ref[l, :, pl.ds(pl.multiple_of(s * width, width), width)] = total[:rows_gu, width:]
            gd_ref[l, pl.ds(pl.multiple_of(s * SHARE, SHARE), SHARE)] = total[rows_gu:]
        wide = total.astype(F32)
        wide = wide * wide
        sq[:, cols] += jnp.sum(wide.reshape(-1, 8, wide.shape[-1]), axis=0)
        for j in range(far):
            rs(q, j, True, narrow).wait_send()
        for j in range(far - 1):
            rs(q, j, False, narrow).wait_send()

    def rs_slot(q, slot):
        j = 4 - slot
        c = q - j
        when(both(c >= 0, c < chunks), lambda: sized(c, lambda narrow: rs_hop(c, j, narrow)))

    def rs_end(q):
        c = q - 3
        when(both(c >= 0, c < chunks), lambda: sized(c, lambda narrow: rs_last(c, narrow)))

    def scale_of(wide):
        return lax.rsqrt(jnp.mean(wide * wide, -1, keepdims=True) + 1e-6)

    def norm_tile(t, src, a, at_):
        wide = src[tile(t)].astype(F32)
        out = (wide * scale_of(wide)).astype(BF16)
        a[tile(t)] = out
        at_[:, tile(t)] = out.T

    def w_gu(u, narrow):
        return w[u, :, :rows_gu, lanes(narrow)].reshape(n * rows_gu, -1)

    def w_d(u, narrow):
        if not narrow:
            return w[u, :, rows_gu:, :].reshape(width, d)
        mid = rows_gu + SHARE // 2
        return jnp.concatenate([w[u, :, rows_gu:mid, :width].reshape(-1, width), w[u, :, mid:, :width].reshape(-1, width)], 1)

    sq[...] = jnp.zeros_like(sq)
    ahead = 3 * far // 2

    def start_tile(t):
        for c in fetch(t):
            c.wait()
        norm_tile(t, h, a0, a0t)
        byt[:, tile(t)] = by[tile(t)].T

    for i in range(ahead + 1):
        stage(i, 0)
        if 1 <= i <= far:
            pl.loop(tiles * (i - 1) // far, tiles * i // far)(start_tile)
        if i < ahead:
            stage(i, 1)

    acc[...] = jnp.zeros_like(acc)

    def forward(s, narrow):
        ready(s, narrow)
        size = BIG
        count, big = cut_by(size)

        @pl.loop(0, count)
        def _(t):
            gu = dot(a0[big(t)], w_gu(s, narrow))
            units = gu.shape[1] // 2
            gate, up = gu[:, :units], gu[:, units:]
            act = gate * (0.5 * jnp.tanh(0.5 * gate) + 0.5) * up
            acc[big(t)] += dot(act.astype(BF16), w_d(s, narrow))
            if not narrow:
                pl.when(jnp.logical_and(s == 0, t == count // 2 - 1))(lambda: stage(ahead, 1))
            pl.when(t == count // 2 - 1)(lambda: stage(s + ahead + 1, 0))
            pl.when(t == count - 1)(lambda: stage(s + ahead + 1, 1))

    @pl.loop(0, steps - 1)
    def _(s):
        forward(s, False)

    forward(steps - 1, True)

    @pl.loop(0, tiles)
    def _(t):
        h[tile(t)] = h[tile(t)] + acc[tile(t)].astype(BF16)
        norm_tile(t, h, a1, a1t)

    def backward(first, a, a_t, whole):
        base = steps if whole else 0
        if whole:
            acc[...] = jnp.zeros_like(acc)

        dgu[...] = jnp.zeros_like(dgu)
        ddt[...] = jnp.zeros_like(ddt)

        def chunk(s, narrow):
            q, u = first + s, base + s
            if whole:
                ready(u, narrow)
            count, big = cut_by(BIG)
            units = width // 2 if narrow else width

            @pl.loop(0, count)
            def _(t):
                gu = dot(a[big(t)], w_gu(u, narrow))
                dact = dot_nt(by[big(t)], w_d(u, narrow)).astype(BF16).astype(F32)
                gate, up = gu[:, :units], gu[:, units:]
                s_ = 0.5 * jnp.tanh(0.5 * gate) + 0.5
                silu = gate * s_
                act = (silu * up).astype(BF16)
                dup = (dact * silu).astype(BF16)
                dgate = (dact * up * (s_ + silu * (1.0 - s_))).astype(BF16)
                both_ = jnp.concatenate([dgate, dup], axis=1)
                dgu[:, : 2 * units] += dot(a_t[:, big(t)], both_)
                ddt[:, :units] += dot(byt[:, big(t)], act)
                if whole:
                    acc[big(t)] += dot_nt(both_, w_gu(u, narrow))
                for slot in (1, 2, 3):

                    @pl.when(t == -(-slot * count // 4) - 1)
                    def _():
                        if whole and slot != 2:
                            for odd in (0, 1):
                                stage(base + ahead + 1 + 2 * s + slot // 2, odd)
                        rs_slot(q, slot)

            rs_end(q)
            p = lax.rem(q, 3)
            part[p, :, :rows_gu, lanes(narrow)] = dgu[:, : 2 * units].astype(BF16).reshape(n, rows_gu, 2 * units)
            down = ddt[:, :units].T.astype(BF16)
            if narrow:
                mid = rows_gu + SHARE // 2
                part[p, :, rows_gu:mid, :width] = down[:, :width].reshape(n, SHARE // 2, width)
                part[p, :, mid:, :width] = down[:, width:].reshape(n, SHARE // 2, width)
            else:
                part[p, :, rows_gu:, :] = down.reshape(n, SHARE, d)
                dgu[...] = jnp.zeros_like(dgu)
                ddt[...] = jnp.zeros_like(ddt)
            rs_hop(q, 0, narrow)
            if narrow and not whole:
                rs_hop(q - 2, 3, False)

        @pl.loop(0, steps - 1)
        def _(s):
            chunk(s, False)

        chunk(steps - 1, True)

    backward(0, a1, a1t, True)

    @pl.loop(0, tiles)
    def _(t):
        wide = h[tile(t)].astype(F32)
        scale = scale_of(wide)
        ct = acc[tile(t)].astype(BF16).astype(F32)
        back = scale * ct - wide * (scale * scale * scale) * jnp.mean(ct * wide, -1, keepdims=True)
        new = by[tile(t)] + back.astype(BF16)
        by[tile(t)] = new
        byt[:, tile(t)] = new.T

    backward(steps, a0, a0t, False)

    for q in range(chunks, chunks + 3):
        for slot in (1, 2, 3)[q == chunks :]:
            rs_slot(q, slot)
        rs_end(q)

    sq_all[me] = jnp.sum(sq[...].reshape(8, -1, 128), axis=1)
    for k in range(1, n):
        pltpu.make_async_remote_copy(
            sq_all.at[me], sq_all.at[me], sq_send.at[k], sq_recv.at[k], device_id={"dp": at(me + k)}, device_id_type=MESH
        ).start()
    for k in range(1, n):
        ref = sq_all.at[at(me - k)]
        c = pltpu.make_async_remote_copy(ref, ref, sq_send.at[k], sq_recv.at[k], device_id={"dp": at(me + k)}, device_id_type=MESH)
        c.wait_recv()
    for k in range(1, n):
        ref = sq_all.at[me]
        pltpu.make_async_remote_copy(ref, ref, sq_send.at[k], sq_recv.at[k], device_id={"dp": at(me + k)}, device_id_type=MESH).wait_send()

    factor = jnp.minimum(1.0, 0.5 * lax.rsqrt(jnp.sum(sq_all[...]) / (n * layers * (2 * rows * hidden + share * d)) + 1e-30))
    f_ref[...] = jnp.full(f_ref.shape, factor)

    def sent(narrow, u):
        for j in range(far):
            ag(u, j, True, narrow).wait_send()
        for j in range(far - 1):
            ag(u, j, False, narrow).wait_send()
        swap(u, narrow).wait_send()

    @pl.loop(0, chunks)
    def _(u):
        sized(u, lambda narrow: sent(narrow, u))


def update(n, f_ref, gg_ref, gu_ref, gd_ref, *refs):
    given, new, held, (in_sem, out_sem) = refs[:9], refs[9:18], refs[18:27], refs[27:]
    layers, rows, hidden = gg_ref.shape
    share = gd_ref.shape[1]

    def fetch(k, l):
        return pltpu.make_async_copy(given[k].at[l], held[k].at[l], in_sem.at[k, l])

    def put(k, l):
        return pltpu.make_async_copy(held[k].at[l], new[k].at[l], out_sem.at[k, l])

    for i in range(3):
        for l in range(layers):
            for k in (i, 3 + i, 6 + i):
                fetch(k, l).start()
    f = lax.broadcasted_iota(jnp.int32, (1, hidden), 1)
    first = f % share // SHARE * SHARE
    to = first * n + f // share * jnp.minimum(SHARE, share - first) + f % share - first
    pick = jnp.where(lax.broadcasted_iota(jnp.int32, (hidden, hidden), 0) == to, 1.0, 0.0).astype(BF16)
    both = jnp.concatenate([gg_ref[...].reshape(layers * rows, hidden), gu_ref[...].reshape(layers * rows, hidden)], 0)
    both = dot(both, pick).reshape(2, layers, rows, hidden)
    factor = f_ref[:1, :1]
    for i in range(3):
        for l in range(layers):
            ks = (i, 3 + i, 6 + i)
            for k in ks:
                fetch(k, l).wait()
            w, m, v = (held[k].at[l] for k in ks)
            g = factor * (gd_ref[l].astype(F32) if i == 2 else both[i, l])
            w[...], m[...], v[...] = adamw(w[...].astype(F32), m[...], v[...], g)
            for k in ks:
                put(k, l).start()
    for k in range(9):
        for l in range(layers):
            put(k, l).wait()


def adamw(w, m, v, g):
    m = 0.9 * m + 0.1 * g
    v = 0.95 * v + 0.05 * g * g
    step = m * lax.rsqrt(v + 1e-8) + 0.1 * w
    return (w - 0.02 * step).astype(BF16), m, v


def solution(mesh):
    n = mesh.shape["dp"]

    def step(x, dy, *arrays):
        w_gate, w_up, w_down = arrays[:3]
        layers, rows, _ = w_gate.shape
        share, d = w_down.shape[1:]
        tokens = x.shape[1]
        steps = -(-share // SHARE)
        width = n * SHARE
        chunks = layers * steps

        slots, hops = 5, n - 1
        dma = pltpu.SemaphoreType.DMA
        g_gate, g_up, g_down, factor = pl.pallas_call(
            functools.partial(kernel, n, steps),
            out_shape=(
                jax.ShapeDtypeStruct((layers, rows, n * share), BF16),
                jax.ShapeDtypeStruct((layers, rows, n * share), BF16),
                jax.ShapeDtypeStruct((layers, share, d), BF16),
                jax.ShapeDtypeStruct((8, 128), F32),
            ),
            in_specs=[pl.BlockSpec(memory_space=pl.ANY)] * 2 + [pl.BlockSpec(memory_space=pltpu.VMEM)] * 3,
            out_specs=(pl.BlockSpec(memory_space=pltpu.VMEM),) * 4,
            scratch_shapes=[
                pltpu.VMEM((tokens, d), BF16),
                pltpu.VMEM((tokens, d), BF16),
                pltpu.VMEM((d, tokens), BF16),
                pltpu.VMEM((tokens, d), BF16),
                pltpu.VMEM((d, tokens), BF16),
                pltpu.VMEM((tokens, d), BF16),
                pltpu.VMEM((d, tokens), BF16),
                pltpu.VMEM((tokens, d), F32),
                pltpu.VMEM((chunks, rows + SHARE, d), BF16),
                pltpu.VMEM((chunks, n, rows + SHARE, d), BF16),
                pltpu.VMEM((3, n, rows + SHARE, d), BF16),
                pltpu.VMEM((slots, hops, rows + SHARE, d), BF16),
                pltpu.VMEM((d, 2 * width), F32),
                pltpu.VMEM((d, width), F32),
                pltpu.VMEM((8, d), F32),
                pltpu.VMEM((n, 8, 128), F32),
                dma((chunks, hops)),
                dma((chunks, hops)),
                dma((chunks,)),
                dma((chunks,)),
                dma,
                dma((2, tokens // TILE)),
                dma((slots, hops)),
                dma((slots, hops)),
                dma((n,)),
                dma((n,)),
            ],
            compiler_params=pltpu.CompilerParams(collective_id=0, has_side_effects=True, vmem_limit_bytes=67043328),
            name="step",
        )(x[0], dy[0], w_gate, w_up, w_down)

        held = [pltpu.VMEM(one.shape, one.dtype) for one in arrays]
        return pl.pallas_call(
            functools.partial(update, n),
            out_shape=tuple(jax.ShapeDtypeStruct(one.shape, one.dtype) for one in arrays),
            in_specs=[pl.BlockSpec(memory_space=pltpu.VMEM)] * 4 + [pl.BlockSpec(memory_space=pl.ANY)] * 9,
            out_specs=(pl.BlockSpec(memory_space=pl.ANY),) * 9,
            scratch_shapes=held + [dma((9, layers)), dma((9, layers))],
            name="update",
        )(factor, g_gate, g_up, g_down, *arrays)

    states, cut = P(("rep", "dp"), None, None), P(None, "dp", None)
    return jax.shard_map(
        step,
        mesh=mesh,
        in_specs=(states, states) + (cut,) * 9,
        out_specs=(P("rep", "dp", None),) * 9,
        check_vma=False,
    )
```
